256 devices in a mesh: blk: 128 (over y, z, x_lo, core), rel: 2 (over x_hi).
Axes of the slice: x: 4 (x_hi: 2, x_lo: 2; x = x_hi * 2 + x_lo), y: 4, z: 8, core: 2. Of those that a mesh axis runs over, the one named last changes fastest.
Arguments:
- user_table: float32 [131072, 512], P(('blk', 'rel')), may hold values from -1.5 to 1.5
- user_accum: float32 [131072], P(('blk', 'rel')), may hold values from 1 to 100
- item_table: float32 [262144, 512], P(('blk', 'rel')), may hold values from -1.5 to 1.5
- item_accum: float32 [262144], P(('blk', 'rel')), may hold values from 1 to 100
- relation: bfloat16 [512, 512], replicated, may hold values from -0.25 to 0.25
- relation_accum: float32 [512], replicated, may hold values from 0.5 to 8
- targets: bfloat16 [2, 131072, 2048], P(None, 'blk', 'rel'), may hold values from 0 to 1
Outputs:
- user_table_next: float32 [131072, 512], P(('blk', 'rel'))
- user_accum_next: float32 [131072], P(('blk', 'rel'))
- item_table_next: float32 [262144, 512], P(('blk', 'rel'))
- item_accum_next: float32 [262144], P(('blk', 'rel'))
- relation_step: float32 [512, 512], replicated
- relation_accum_next: float32 [512], replicated
The draws below stay inside these ranges and needn't reach their ends.
All inputs are finite; a program needn't handle non-finite values.
Results may differ from the reference program's by a relative error of at most 0.0037.
The reference program's roundings to bfloat16 on the way count: a program that leaves them out, or rounds other values in their place, can miss the bound.
Values may be sent and summed in bfloat16 or wider, within the bound.
A program may use at most 64 MiB of HBM per device.

```python
import math
import jax
import jax.numpy as jnp
from jax import lax

D = 512
U_ROWS = 1024
I_ROWS = 2048
ROUNDS = 2
NB = 128
NU = 131072
NI = 262144


def levels(stream_key, dims, cuts, low, top_value):
    def one(dim, blocks):
        draws = jax.random.uniform(jax.random.fold_in(jax.random.fold_in(stream_key, 6), dim), (blocks,), jnp.float32, low / len(cuts), top_value / len(cuts))
        return jnp.repeat(jnp.exp(draws), dims[dim] // blocks).reshape((-1,) + (1,) * (len(dims) - dim - 1))

    level = one(*cuts[0])
    for cut in cuts[1:]:
        level = level * one(*cut)
    return level


def normal_values(stream_key, dims, spread, most, cuts=(), dtype=jnp.bfloat16):
    loudness = levels(stream_key, dims, cuts, -0.22, 0.18) if cuts else 1.0
    entries = jax.random.normal(stream_key, dims, jnp.float32) * spread * loudness
    return jnp.minimum(jnp.maximum(entries, -most), most).astype(dtype)


def setup_inputs(seed: int = 0) -> dict:
    key_list = jax.random.split(jax.random.key(seed), 8)
    user_table = normal_values(key_list[0], (NU, D), 0.25, 1.5, ((0, 256),), jnp.float32)
    user_accum = jnp.clip(jnp.exp(math.log(100.0) - 4.6051702 * jax.random.uniform(key_list[1], (NU,), jnp.float32) ** levels(key_list[1], (NU,), ((0, 256),), -0.2, 0.2)), 1.0, 100.0)
    item_table = normal_values(key_list[2], (NI, D), 0.25, 1.5, ((0, 256),), jnp.float32)
    item_accum = jnp.clip(jnp.exp(math.log(100.0) - 4.6051702 * jax.random.uniform(key_list[3], (NI,), jnp.float32) ** levels(key_list[3], (NI,), ((0, 256),), -0.2, 0.2)), 1.0, 100.0)
    relation = normal_values(key_list[4], (D, D), D ** -0.5, 0.25)
    relation_accum = jnp.clip(jnp.exp(jax.random.uniform(key_list[5], (D,), jnp.float32, math.log(0.5), math.log(8.0))), 0.5, 8.0)
    targets = jnp.clip(1.0 * jax.random.uniform(key_list[6], (ROUNDS, NU, I_ROWS), jnp.float32) ** levels(key_list[6], (ROUNDS, NU, I_ROWS), ((1, 128), (2, 2)), -0.2, 0.2), 0.0, 1.0).astype(jnp.bfloat16)
    return dict(user_table=user_table, user_accum=user_accum, item_table=item_table, item_accum=item_accum, relation=relation, relation_accum=relation_accum, targets=targets)


learn_rate = 0.1
epsilon = 1e-06

def adagrad_rows(table, accum, grads):
    accum_next = accum + lax.optimization_barrier(jnp.mean(grads * grads, axis=1))
    return (table - learn_rate * grads * lax.rsqrt(accum_next + epsilon)[:, None], accum_next)

def reference(user_table, user_accum, item_table, item_accum, relation, relation_accum, targets):
    user_parts = user_table.reshape(NB, U_ROWS, D)
    user_sums = user_accum.reshape(NB, U_ROWS)
    item_parts = item_table.reshape(NB, I_ROWS, D)
    item_sums = item_accum.reshape(NB, I_ROWS)
    label_parts = targets.reshape(ROUNDS, NB, U_ROWS, I_ROWS)
    total = jnp.zeros((D, D), jnp.float32)

    def bucket(carry, inputs):
        users, uacc, items, iacc, labels_now = inputs
        user_bf = users.astype(jnp.bfloat16)
        item_bf = items.astype(jnp.bfloat16)
        anchor = jnp.dot(user_bf, relation, preferred_element_type=jnp.float32).astype(jnp.bfloat16)
        scores = jnp.dot(anchor, item_bf.T, preferred_element_type=jnp.float32)
        errors = (jax.nn.sigmoid(scores) - labels_now.astype(jnp.float32)).astype(jnp.bfloat16)
        mapped = jnp.dot(item_bf, relation.T, preferred_element_type=jnp.float32).astype(jnp.bfloat16)
        user_grad = jnp.dot(errors, mapped, preferred_element_type=jnp.float32)
        item_grad = jnp.dot(errors.T, anchor, preferred_element_type=jnp.float32)
        crossed = jnp.dot(user_bf.T, errors, preferred_element_type=jnp.float32).astype(jnp.bfloat16)
        carry = carry + jnp.dot(crossed, item_bf, preferred_element_type=jnp.float32)
        users_new, uacc_new = adagrad_rows(users, uacc, user_grad)
        items_new, iacc_new = adagrad_rows(items, iacc, item_grad)
        return (carry, (users_new, uacc_new, items_new, iacc_new))
    for turn in range(ROUNDS):
        total, (user_parts, user_sums, item_parts, item_sums) = lax.scan(bucket, total, (user_parts, user_sums, item_parts, item_sums, label_parts[turn]))
        item_parts = jnp.roll(item_parts, 1, axis=0)
        item_sums = jnp.roll(item_sums, 1, axis=0)
    mean_grad = total / (NB * ROUNDS)
    accum_next = relation_accum + lax.optimization_barrier(jnp.mean(mean_grad * mean_grad, axis=1))
    relation_step = mean_grad * lax.rsqrt(accum_next + epsilon)[:, None]
    return (user_parts.reshape(NU, D), user_sums.reshape(NU), item_parts.reshape(NI, D), item_sums.reshape(NI), relation_step, accum_next)
```

```python
import jax
import jax.numpy as jnp
from jax import lax
from jax.experimental import pallas as pl
from jax.experimental.pallas import tpu as pltpu
from jax.sharding import PartitionSpec as P

learn_rate = 0.1
epsilon = 1e-06

MESH = pl.DeviceIdType.MESH
D = 512
UH = 512
IH = 1024
NB = 128
ROUNDS = 2
UC = 128
IC = 256
BF = jnp.bfloat16
F32 = jnp.float32


def mm(a, b, ca, cb):
    return lax.dot_general(a, b, (((ca,), (cb,)), ((), ())), preferred_element_type=F32)


def to_columns(rows, cols):
    for i in range(rows.shape[0]):
        cols[i * 128 : (i + 1) * 128, :] = jnp.broadcast_to(rows[i : i + 1, :], (128, 128)).T


def to_rows(cols, rows):
    for i in range(rows.shape[0]):
        rows[i : i + 1, :] = cols[i * 128 : (i + 1) * 128, :].T[0:1, :]


def adagrad(table, accum, grads):
    accum_next = accum + jnp.mean(grads * grads, axis=1, keepdims=True)
    return table - learn_rate * grads * lax.rsqrt(accum_next + epsilon), accum_next


def kernel(
    user_in, uacc_in, item_in, iacc_in, rel_in, racc_in, tgt_in,
    user_out, uacc_out, item_out, iacc_out, step_out, racc_out,
    users, uacc, items0, items1, items2, iacc0, iacc1, iacc2, rel, racc, tgt0, tgt1,
    ub0, ub1, vb0, vb1, vb2, vtx0, vtx1, anchor, errors, wsum, ugown,
    gtx0, gtx1, grx0, grx1, ucol, icol, rcol, term, rcore, ry, rz, rx, total,
    load, store, usend, urecv, gsend, grecv, isend, irecv, asend, arecv,
    csend, crecv, ysend, yrecv, zsend, zrecv, xsend, xrecv,
):
    b = lax.axis_index("blk")
    r = lax.axis_index("rel")
    core = lax.rem(b, 2)
    xlo = lax.rem(b // 2, 2)
    z = lax.rem(b // 4, 8)
    y = b // 32
    x = 2 * r + xlo
    partner = (b, 1 - r)
    sibling = (b + 1 - 2 * core, r)
    other = (lax.rem(b + 2 * core + (NB - 1), NB), r)
    nxt = (lax.rem(b + 1, NB), r)

    def xpeer(d):
        xp = lax.rem(x + d, 4)
        return (b - 2 * xlo + 2 * lax.rem(xp, 2), xp // 2)

    def ypeer(d):
        return (b - 32 * y + 32 * lax.rem(y + d, 4), r)

    def zpeer(d):
        return (b - 4 * z + 4 * lax.rem(z + d, 8), r)

    barrier = pltpu.get_barrier_semaphore()
    greet = [xpeer(d) for d in range(1, 4)] + [ypeer(d) for d in range(1, 4)]
    greet += [zpeer(d) for d in range(1, 8)] + [sibling, other]
    for peer in greet:
        pl.semaphore_signal(barrier, inc=1, device_id=peer, device_id_type=MESH)

    loads = []
    for src, dst in (
        (user_in, users), (rel_in, rel), (item_in, items0), (tgt_in.at[0], tgt0),
        (uacc_in, uacc), (iacc_in, iacc0), (racc_in, racc), (tgt_in.at[1], tgt1),
    ):
        copy = pltpu.make_async_copy(src, dst, load.at[len(loads)])
        copy.start()
        loads.append(copy)

    own = pl.multiple_of(r * UH, UH)
    far = pl.multiple_of((1 - r) * UH, UH)

    ubs, vbs, vtxs = (ub0, ub1), (vb0, vb1), (vtx0, vtx1)
    tgts, gtxs, grxs = (tgt0, tgt1), (gtx0, gtx1), (grx0, grx1)
    itabs, iaccs, vins = (items0, items1, items2), (iacc0, iacc1, iacc2), (vb0, vb1, vb2)

    def user_copy(turn, k, src0, dst0):
        return pltpu.make_async_remote_copy(
            ubs[turn].at[pl.ds(src0 + k * UC, UC)], ubs[turn].at[pl.ds(dst0 + k * UC, UC)],
            usend.at[turn, k], urecv.at[turn, k], device_id=partner, device_id_type=MESH,
        )

    def grad_copy(turn, k):
        rows = pl.ds(k * UC, UC)
        return pltpu.make_async_remote_copy(
            gtxs[turn].at[rows], grxs[turn].at[rows],
            gsend.at[turn, k], grecv.at[turn, k], device_id=partner, device_id_type=MESH,
        )

    def item_copy_wide(turn, k, src):
        rows = pl.ds(k * IC, IC)
        return pltpu.make_async_remote_copy(
            src.at[rows], itabs[turn + 1].at[rows],
            isend.at[turn, k], irecv.at[turn, k], device_id=nxt, device_id_type=MESH,
        )

    def item_copy(turn, k):
        rows = pl.ds(k * IC, IC)
        return pltpu.make_async_remote_copy(
            vtxs[turn].at[rows], vins[turn + 1].at[rows],
            isend.at[turn, k], irecv.at[turn, k], device_id=nxt, device_id_type=MESH,
        )

    def accum_copy(turn, src):
        return pltpu.make_async_remote_copy(
            src, iaccs[turn + 1], asend.at[turn], arecv.at[turn],
            device_id=nxt, device_id_type=MESH,
        )

    def score_rows(turn, row0, n):
        rows = pl.ds(row0, n)
        anc = mm(ubs[turn][rows, :], rel[...], 1, 0).astype(BF)
        anchor[rows, :] = anc
        scores = mm(anc, vbs[turn][...], 1, 1)
        err = (0.5 * jnp.tanh(0.5 * scores) + 0.5 - tgts[turn][rows, :].astype(F32)).astype(BF)
        errors[rows, :] = err
        w = mm(err, vbs[turn][...], 1, 0).astype(BF)
        wsum[rows, :] = w
        return mm(w, rel[...], 1, 1)

    def own_rows(turn):
        def step(k, carry):
            row0 = pl.multiple_of(k * 256, 256)
            ugown[pl.ds(row0, 256), :] = score_rows(turn, pl.multiple_of(own + row0, 256), 256)
            return carry

        lax.fori_loop(0, UH // 256, step, 0)

    def far_rows(turn):
        def step(k, carry):
            user_copy(turn, k, own, far).wait_recv()
            row0 = pl.multiple_of(k * UC, UC)
            grad = score_rows(turn, pl.multiple_of(far + row0, UC), UC)
            gtxs[turn][pl.ds(row0, UC), :] = grad.astype(BF)
            grad_copy(turn, k).start()
            return carry

        lax.fori_loop(0, UH // UC, step, 0)

    def add_term(turn, row0, first):
        rows = pl.ds(row0, UH)
        part = mm(ubs[turn][rows, :], wsum[rows, :], 0, 0)
        term[...] = part if first else term[...] + part

    def item_chunk(turn, k):
        rows = pl.ds(k * IC, IC)
        grad = mm(errors[:, k * IC : (k + 1) * IC], anchor[...], 0, 0)
        new, acc = adagrad(itabs[turn][rows, :], icol[rows, 0:1], grad)
        icol[rows, :] = jnp.broadcast_to(acc, (IC, 128))
        itabs[turn][rows, :] = new
        vtxs[turn][rows, :] = new.astype(BF)

        @pl.when(core == 0)
        def _():
            item_copy_wide(turn, k, itabs[turn]).start()

        @pl.when(core == 1)
        def _():
            item_copy(turn, k).start()

    def user_chunks(turn):
        def step(k, carry):
            grad_copy(turn, k).wait_recv()
            row0 = pl.multiple_of(k * UC, UC)
            rows = pl.ds(row0, UC)
            grad = ugown[rows, :] + grxs[turn][rows, :].astype(F32)
            new, acc = adagrad(users[rows, :], ucol[rows, 0:1], grad)
            ucol[rows, :] = jnp.broadcast_to(acc, (UC, 128))
            users[rows, :] = new
            if turn + 1 < ROUNDS:
                ubs[turn + 1][pl.ds(pl.multiple_of(own + row0, UC), UC), :] = new.astype(BF)
                user_copy(turn + 1, k, own, own).start()
            return carry

        lax.fori_loop(0, UH // UC, step, 0)

    def items_arrive(turn):
        def step(k, carry):
            row0 = pl.multiple_of(k * IC, IC)
            rows = pl.ds(row0, IC)

            @pl.when(core == 0)
            def _():
                item_copy(turn, k).wait_recv()
                itabs[turn + 1][rows, :] = vins[turn + 1][rows, :].astype(F32)

            @pl.when(core == 1)
            def _():
                item_copy_wide(turn, k, itabs[turn]).wait_recv()
                if turn + 1 < ROUNDS:
                    vins[turn + 1][rows, :] = itabs[turn + 1][rows, :].astype(BF)

            return carry

        lax.fori_loop(0, IH // IC, step, 0)
        accum_copy(turn, iaccs[turn]).wait_recv()

    loads[0].wait()
    ub0[pl.ds(own, UH), :] = users[...].astype(BF)
    pl.semaphore_wait(barrier, len(greet))
    for k in range(UH // UC):
        user_copy(0, k, own, own).start()
    for copy in loads[1:7]:
        copy.wait()
    vb0[...] = items0[...].astype(BF)
    to_columns(uacc, ucol)
    to_columns(iacc0, icol)
    to_columns(racc, rcol)
    own_rows(0)
    add_term(0, own, True)
    far_rows(0)
    for k in range(IH // IC):
        item_chunk(0, k)
    to_rows(icol, iacc0)
    accum_copy(0, iacc0).start()
    user_chunks(0)
    add_term(0, far, False)
    loads[7].wait()

    items_arrive(0)
    to_columns(iacc1, icol)
    own_rows(1)
    add_term(1, own, False)
    far_rows(1)
    add_term(1, far, False)

    half = pl.multiple_of(core * 256, 256)
    away = pl.multiple_of(256 - core * 256, 256)
    base_y = pl.multiple_of(half + y * 64, 64)
    base_z = pl.multiple_of(base_y + z * 8, 8)

    core_copy = pltpu.make_async_remote_copy(
        term.at[pl.ds(away, 256)], rcore, csend.at[0], crecv.at[0],
        device_id=sibling, device_id_type=MESH,
    )
    core_copy.start()
    item_chunk(1, 0)
    core_copy.wait_recv()
    term[pl.ds(half, 256), :] = term[pl.ds(half, 256), :] + rcore[...]
    y_copies = []
    for d in range(1, 4):
        piece = pl.multiple_of(half + lax.rem(y + d, 4) * 64, 64)
        y_copies.append(pltpu.make_async_remote_copy(
            term.at[pl.ds(piece, 64)], ry.at[d - 1], ysend.at[d - 1], yrecv.at[d - 1],
            device_id=ypeer(d), device_id_type=MESH,
        ))
        y_copies[-1].start()
    item_chunk(1, 1)
    item_chunk(1, 2)
    for copy in y_copies:
        copy.wait_recv()
    term[pl.ds(base_y, 64), :] = term[pl.ds(base_y, 64), :] + ry[0] + ry[1] + ry[2]
    z_copies = []
    for d in range(1, 8):
        piece = pl.multiple_of(base_y + lax.rem(z + d, 8) * 8, 8)
        z_copies.append(pltpu.make_async_remote_copy(
            term.at[pl.ds(piece, 8)], rz.at[d - 1], zsend.at[d - 1], zrecv.at[d - 1],
            device_id=zpeer(d), device_id_type=MESH,
        ))
        z_copies[-1].start()
    item_chunk(1, 3)
    to_rows(icol, iacc1)
    accum_copy(1, iacc1).start()
    for copy in z_copies:
        copy.wait_recv()
    part = term[pl.ds(base_z, 8), :]
    for d in range(7):
        part = part + rz[d]
    rx[pl.ds(x, 1)] = part[None]
    x_sends, x_recvs = [], []
    for d in range(1, 4):
        args = dict(send_sem=xsend.at[d - 1], recv_sem=xrecv.at[d - 1],
                    device_id=xpeer(d), device_id_type=MESH)
        x_sends.append(pltpu.make_async_remote_copy(rx.at[x], rx.at[x], **args))
        x_recvs.append(pltpu.make_async_remote_copy(rx.at[x], rx.at[lax.rem(x + 4 - d, 4)], **args))
        x_sends[-1].start()

    user_chunks(1)
    to_rows(ucol, uacc)
    stores = [
        pltpu.make_async_copy(users, user_out, store.at[0]),
        pltpu.make_async_copy(uacc, uacc_out, store.at[1]),
    ]
    for copy in stores:
        copy.start()

    for copy in x_recvs:
        copy.wait_recv()
    total[pl.ds(base_z, 8), :] = rx[0] + rx[1] + rx[2] + rx[3]

    def spread(src0, dst0, n, sends, recvs, k, peer):
        return pltpu.make_async_remote_copy(
            total.at[pl.ds(src0, n)], total.at[pl.ds(dst0, n)], sends.at[k], recvs.at[k],
            device_id=peer, device_id_type=MESH,
        )

    back = []
    for d in range(1, 8):
        back.append(spread(base_z, base_z, 8, zsend, zrecv, 6 + d, zpeer(d)))
        back[-1].start()
    for d in range(1, 8):
        src = pl.multiple_of(base_y + lax.rem(z + 8 - d, 8) * 8, 8)
        spread(base_z, src, 8, zsend, zrecv, 6 + d, zpeer(d)).wait_recv()
    for d in range(1, 4):
        back.append(spread(base_y, base_y, 64, ysend, yrecv, 2 + d, ypeer(d)))
        back[-1].start()
    for d in range(1, 4):
        src = pl.multiple_of(half + lax.rem(y + 4 - d, 4) * 64, 64)
        spread(base_y, src, 64, ysend, yrecv, 2 + d, ypeer(d)).wait_recv()
    back.append(spread(half, half, 256, csend, crecv, 1, sibling))
    back[-1].start()

    items_arrive(1)
    for src, dst in ((items2, item_out), (iacc2, iacc_out)):
        stores.append(pltpu.make_async_copy(src, dst, store.at[len(stores)]))
        stores[-1].start()

    spread(half, away, 256, csend, crecv, 1, sibling).wait_recv()
    mean_grad = total[...] * (1.0 / (NB * ROUNDS))
    step, racc_next = relation_rows(mean_grad, rcol[:, 0:1])
    ugown[...] = step
    rcol[...] = jnp.broadcast_to(racc_next, (D, 128))
    to_rows(rcol, racc)
    for src, dst in ((ugown, step_out), (racc, racc_out)):
        stores.append(pltpu.make_async_copy(src, dst, store.at[len(stores)]))

    for turn in range(ROUNDS):
        for k in range(UH // UC):
            user_copy(turn, k, own, own).wait_send()
            grad_copy(turn, k).wait_send()
        for k in range(IH // IC):

            @pl.when(core == 0)
            def _():
                item_copy_wide(turn, k, itabs[turn]).wait_send()

            @pl.when(core == 1)
            def _():
                item_copy(turn, k).wait_send()

        accum_copy(turn, iaccs[turn]).wait_send()
    for copy in [core_copy] + y_copies + z_copies + x_sends + back:
        copy.wait_send()
    for copy in stores[4:]:
        copy.start()
    for copy in stores:
        copy.wait()


def relation_rows(mean_grad, accum):
    accum_next = accum + jnp.mean(mean_grad * mean_grad, axis=1, keepdims=True)
    return mean_grad * lax.rsqrt(accum_next + epsilon), accum_next


def per_device(user_table, user_accum, item_table, item_accum, relation, relation_accum, targets):
    V = pltpu.VMEM
    dma = lambda *shape: pltpu.SemaphoreType.DMA(shape)
    shapes = [
        ((UH, D), F32), ((4, 128), F32), ((IH, D), F32), ((8, 128), F32), ((D, D), F32), ((4, 128), F32),
    ]
    outs = pl.pallas_call(
        kernel,
        out_shape=[jax.ShapeDtypeStruct(s, t) for s, t in shapes],
        in_specs=[pl.BlockSpec(memory_space=pl.ANY)] * 7,
        out_specs=[pl.BlockSpec(memory_space=pl.ANY)] * 6,
        scratch_shapes=[
            V((UH, D), F32), V((4, 128), F32), V((IH, D), F32), V((IH, D), F32), V((IH, D), F32),
            V((8, 128), F32), V((8, 128), F32), V((8, 128), F32), V((D, D), BF), V((4, 128), F32),
            V((2 * UH, IH), BF), V((2 * UH, IH), BF),
            V((2 * UH, D), BF), V((2 * UH, D), BF), V((IH, D), BF), V((IH, D), BF), V((IH, D), BF),
            V((IH, D), BF), V((IH, D), BF), V((2 * UH, D), BF), V((2 * UH, IH), BF),
            V((2 * UH, D), BF), V((UH, D), F32),
            V((UH, D), BF), V((UH, D), BF), V((UH, D), BF), V((UH, D), BF),
            V((UH, 128), F32), V((IH, 128), F32), V((D, 128), F32), V((D, D), F32),
            V((256, D), F32), V((3, 64, D), F32), V((7, 8, D), F32), V((4, 8, D), F32), V((D, D), F32),
            dma(8), dma(6), dma(2, 4), dma(2, 4), dma(2, 4), dma(2, 4), dma(2, 4), dma(2, 4), dma(2), dma(2),
            dma(2), dma(2), dma(6), dma(6), dma(14), dma(14), dma(3), dma(3),
        ],
        compiler_params=pltpu.CompilerParams(
            collective_id=0, has_side_effects=True, vmem_limit_bytes=60 * 2**20
        ),
    )(
        user_table, user_accum.reshape(4, 128), item_table, item_accum.reshape(8, 128),
        relation, relation_accum.reshape(4, 128), targets,
    )
    users, uacc, items, iacc, step, racc = outs
    return users, uacc.reshape(UH), items, iacc.reshape(IH), step, racc.reshape(D)


def solution(mesh):
    return jax.shard_map(
        per_device,
        mesh=mesh,
        in_specs=(
            P(("blk", "rel"), None),
            P(("blk", "rel")),
            P(("blk", "rel"), None),
            P(("blk", "rel")),
            P(),
            P(),
            P(None, "blk", "rel"),
        ),
        out_specs=(
            P(("blk", "rel"), None),
            P(("blk", "rel")),
            P(("blk", "rel"), None),
            P(("blk", "rel")),
            P(),
            P(),
        ),
        check_vma=False,
    )
```

```python
import jax
import jax.numpy as jnp
from jax import lax
from jax.experimental import pallas as pl
from jax.experimental.pallas import tpu as pltpu
from jax.sharding import PartitionSpec as P

learn_rate = 0.1
epsilon = 1e-06

MESH = pl.DeviceIdType.MESH
D = 512
UH = 512
IH = 1024
NB = 128
ROUNDS = 2
UC = 128
IC = 256
BF = jnp.bfloat16
F32 = jnp.float32
SCATTER = F32
GATHER = F32


def mm(a, b, ca, cb):
    return lax.dot_general(a, b, (((ca,), (cb,)), ((), ())), preferred_element_type=F32)


def to_columns(rows, cols):
    for i in range(rows.shape[0]):
        cols[i * 128 : (i + 1) * 128, :] = jnp.broadcast_to(rows[i : i + 1, :], (128, 128)).T


def to_rows(cols, rows):
    for i in range(rows.shape[0]):
        rows[i : i + 1, :] = cols[i * 128 : (i + 1) * 128, :].T[0:1, :]


def adagrad(table, accum, grads):
    accum_next = accum + jnp.mean(grads * grads, axis=1, keepdims=True)
    return table - learn_rate * grads * lax.rsqrt(accum_next + epsilon), accum_next


def kernel(
    user_in, uacc_in, item_in, iacc_in, rel_in, tgt_in,
    user_out, uacc_out, item_out, iacc_out, total_out,
    users, uacc, items0, items1, items2, iacc0, iacc1, iacc2, rel, tgt0, tgt1,
    ub0, ub1, vb0, vb1, vb2, vtx0, vtx1, anchor, errors, wsum, ugown,
    gtx0, gtx1, grx0, grx1, ucol, icol, term, rcore, mine, ry, sumy, rz, rx, sumz, total,
    load, usend, urecv, gsend, grecv, isend, irecv, asend, arecv,
    csend, crecv, ysend, yrecv, zsend, zrecv, xsend, xrecv,
):
    b = lax.axis_index("blk")
    r = lax.axis_index("rel")
    core = lax.rem(b, 2)
    xlo = lax.rem(b // 2, 2)
    z = lax.rem(b // 4, 8)
    y = b // 32
    x = 2 * r + xlo
    partner = (b, 1 - r)
    sibling = (b + 1 - 2 * core, r)
    other = (lax.rem(b + 2 * core + (NB - 1), NB), r)
    nxt = (lax.rem(b + 1, NB), r)

    def xpeer(d):
        xp = lax.rem(x + d, 4)
        return (b - 2 * xlo + 2 * lax.rem(xp, 2), xp // 2)

    def ypeer(d):
        return (b - 32 * y + 32 * lax.rem(y + d, 4), r)

    def zpeer(d):
        return (b - 4 * z + 4 * lax.rem(z + d, 8), r)

    barrier = pltpu.get_barrier_semaphore()
    greet = [xpeer(d) for d in range(1, 4)] + [ypeer(d) for d in range(1, 4)]
    greet += [zpeer(d) for d in range(1, 8)] + [sibling, other]
    for peer in greet:
        pl.semaphore_signal(barrier, inc=1, device_id=peer, device_id_type=MESH)

    loads = []
    for src, dst in (
        (user_in, users), (rel_in, rel), (item_in, items0), (tgt_in.at[0], tgt0),
        (uacc_in, uacc), (iacc_in, iacc0), (tgt_in.at[1], tgt1),
    ):
        copy = pltpu.make_async_copy(src, dst, load.at[len(loads)])
        copy.start()
        loads.append(copy)

    own = pl.multiple_of(r * UH, UH)
    far = pl.multiple_of((1 - r) * UH, UH)

    ubs, vbs, vtxs = (ub0, ub1), (vb0, vb1), (vtx0, vtx1)
    tgts, gtxs, grxs = (tgt0, tgt1), (gtx0, gtx1), (grx0, grx1)
    itabs, iaccs, vins = (items0, items1, items2), (iacc0, iacc1, iacc2), (vb0, vb1, vb2)

    def user_copy(turn, k, src0, dst0):
        return pltpu.make_async_remote_copy(
            ubs[turn].at[pl.ds(src0 + k * UC, UC)], ubs[turn].at[pl.ds(dst0 + k * UC, UC)],
            usend.at[turn, k], urecv.at[turn, k], device_id=partner, device_id_type=MESH,
        )

    def grad_copy(turn, k):
        rows = pl.ds(k * UC, UC)
        return pltpu.make_async_remote_copy(
            gtxs[turn].at[rows], grxs[turn].at[rows],
            gsend.at[turn, k], grecv.at[turn, k], device_id=partner, device_id_type=MESH,
        )

    def item_copy_wide(turn, k, src):
        rows = pl.ds(k * IC, IC)
        return pltpu.make_async_remote_copy(
            src.at[rows], itabs[turn + 1].at[rows],
            isend.at[turn, k], irecv.at[turn, k], device_id=nxt, device_id_type=MESH,
        )

    def item_copy(turn, k):
        rows = pl.ds(k * IC, IC)
        return pltpu.make_async_remote_copy(
            vtxs[turn].at[rows], vins[turn + 1].at[rows],
            isend.at[turn, k], irecv.at[turn, k], device_id=nxt, device_id_type=MESH,
        )

    def accum_copy(turn, src):
        return pltpu.make_async_remote_copy(
            src, iaccs[turn + 1], asend.at[turn], arecv.at[turn],
            device_id=nxt, device_id_type=MESH,
        )

    def score_rows(turn, row0, n):
        rows = pl.ds(row0, n)
        anc = mm(ubs[turn][rows, :], rel[...], 1, 0).astype(BF)
        anchor[rows, :] = anc
        scores = mm(anc, vbs[turn][...], 1, 1)
        err = (0.5 * jnp.tanh(0.5 * scores) + 0.5 - tgts[turn][rows, :].astype(F32)).astype(BF)
        errors[rows, :] = err
        w = mm(err, vbs[turn][...], 1, 0).astype(BF)
        wsum[rows, :] = w
        return mm(w, rel[...], 1, 1)

    def own_rows(turn):
        def step(k, carry):
            row0 = pl.multiple_of(k * 256, 256)
            ugown[pl.ds(row0, 256), :] = score_rows(turn, pl.multiple_of(own + row0, 256), 256)
            return carry

        lax.fori_loop(0, UH // 256, step, 0)

    def far_rows(turn):
        def step(k, carry):
            user_copy(turn, k, own, far).wait_recv()
            row0 = pl.multiple_of(k * UC, UC)
            grad = score_rows(turn, pl.multiple_of(far + row0, UC), UC)
            gtxs[turn][pl.ds(row0, UC), :] = grad.astype(BF)
            grad_copy(turn, k).start()
            return carry

        lax.fori_loop(0, UH // UC, step, 0)

    def add_term(turn, row0, first):
        rows = pl.ds(row0, UH)
        part = mm(ubs[turn][rows, :], wsum[rows, :], 0, 0)
        term[...] = part if first else term[...] + part

    def item_update(turn, k):
        rows = pl.ds(k * IC, IC)
        grad = mm(errors[:, k * IC : (k + 1) * IC], anchor[...], 0, 0)
        new, acc = adagrad(itabs[turn][rows, :], icol[rows, 0:1], grad)
        icol[rows, :] = jnp.broadcast_to(acc, (IC, 128))
        itabs[turn][rows, :] = new
        vtxs[turn][rows, :] = new.astype(BF)

    def item_send(turn, k):
        @pl.when(core == 0)
        def _():
            item_copy_wide(turn, k, itabs[turn]).start()

        @pl.when(core == 1)
        def _():
            item_copy(turn, k).start()

    def user_chunks(turn):
        def step(k, carry):
            grad_copy(turn, k).wait_recv()
            row0 = pl.multiple_of(k * UC, UC)
            rows = pl.ds(row0, UC)
            grad = ugown[rows, :] + grxs[turn][rows, :].astype(F32)
            new, acc = adagrad(users[rows, :], ucol[rows, 0:1], grad)
            ucol[rows, :] = jnp.broadcast_to(acc, (UC, 128))
            users[rows, :] = new
            if turn + 1 < ROUNDS:
                ubs[turn + 1][pl.ds(pl.multiple_of(own + row0, UC), UC), :] = new.astype(BF)
                user_copy(turn + 1, k, own, own).start()
            return carry

        lax.fori_loop(0, UH // UC, step, 0)

    def items_arrive(turn):
        def step(k, carry):
            row0 = pl.multiple_of(k * IC, IC)
            rows = pl.ds(row0, IC)

            @pl.when(core == 0)
            def _():
                item_copy(turn, k).wait_recv()
                itabs[turn + 1][rows, :] = vins[turn + 1][rows, :].astype(F32)

            @pl.when(core == 1)
            def _():
                item_copy_wide(turn, k, itabs[turn]).wait_recv()
                if turn + 1 < ROUNDS:
                    vins[turn + 1][rows, :] = itabs[turn + 1][rows, :].astype(BF)

            return carry

        lax.fori_loop(0, IH // IC, step, 0)
        accum_copy(turn, iaccs[turn]).wait_recv()

    loads[0].wait()
    ub0[pl.ds(own, UH), :] = users[...].astype(BF)
    pl.semaphore_wait(barrier, len(greet))
    for k in range(UH // UC):
        user_copy(0, k, own, own).start()
    for copy in loads[1:6]:
        copy.wait()
    vb0[...] = items0[...].astype(BF)
    to_columns(uacc, ucol)
    to_columns(iacc0, icol)
    own_rows(0)
    add_term(0, own, True)
    far_rows(0)
    for k in range(IH // IC):
        item_update(0, k)
        item_send(0, k)
    to_rows(icol, iacc0)
    accum_copy(0, iacc0).start()
    user_chunks(0)
    add_term(0, far, False)
    loads[6].wait()

    items_arrive(0)
    to_columns(iacc1, icol)
    own_rows(1)
    add_term(1, own, False)
    far_rows(1)
    add_term(1, far, False)

    half = pl.multiple_of(core * 256, 256)
    away = pl.multiple_of(256 - core * 256, 256)
    base_y = pl.multiple_of(y * 64, 64)
    base_z = pl.multiple_of(z * 8, 8)
    started = []

    def remote(src, dst, sends, recvs, k, peer):
        return pltpu.make_async_remote_copy(
            src, dst, sends.at[k], recvs.at[k], device_id=peer, device_id_type=MESH
        )

    def go(copies):
        for copy in copies:
            copy.start()
        started.extend(copies)
        return copies

    halves = range(2)
    cols = [pl.ds(h * 256, 256) for h in halves]
    core_in = go([
        remote(term.at[pl.ds(away, 256), cols[h]], rcore.at[:, cols[h]], csend, crecv, h, sibling)
        for h in halves
    ])
    item_update(1, 0)
    item_send(1, 0)
    y_in = []
    for h in halves:
        core_in[h].wait_recv()
        both = term[pl.ds(half, 256), cols[h]] + rcore[:, cols[h]]
        mine[:, cols[h]] = both.astype(mine.dtype)
        y_in.append(go([
            remote(
                mine.at[pl.ds(pl.multiple_of(lax.rem(y + d, 4) * 64, 64), 64), cols[h]],
                ry.at[d - 1, :, cols[h]], ysend, yrecv, 3 * h + d - 1, ypeer(d),
            )
            for d in range(1, 4)
        ]))
    item_update(1, 1)
    item_send(1, 1)
    item_update(1, 2)
    item_update(1, 3)
    to_rows(icol, iacc1)
    accum_copy(1, iacc1).start()
    z_in = []
    for h in halves:
        for copy in y_in[h]:
            copy.wait_recv()
        part = mine[pl.ds(base_y, 64), cols[h]].astype(F32)
        for d in range(3):
            part = part + ry[d, :, cols[h]].astype(F32)
        sumy[:, cols[h]] = part
        z_in.append(go([
            remote(
                sumy.at[pl.ds(pl.multiple_of(lax.rem(z + d, 8) * 8, 8), 8), cols[h]],
                rz.at[d - 1, :, cols[h]], zsend, zrecv, 7 * h + d - 1, zpeer(d),
            )
            for d in range(1, 8)
        ]))
    x_in = []
    for h in halves:
        for copy in z_in[h]:
            copy.wait_recv()
        part = sumy[pl.ds(base_z, 8), cols[h]]
        for d in range(7):
            part = part + rz[d, :, cols[h]]
        rx[pl.ds(x, 1), :, cols[h]] = part[None]
        go([
            remote(rx.at[x, :, cols[h]], rx.at[x, :, cols[h]], xsend, xrecv, 3 * h + d - 1, xpeer(d))
            for d in range(1, 4)
        ])
        x_in.append([
            remote(
                rx.at[x, :, cols[h]], rx.at[lax.rem(x + 4 - d, 4), :, cols[h]],
                xsend, xrecv, 3 * h + d - 1, xpeer(d),
            )
            for d in range(1, 4)
        ])
    item_send(1, 2)
    item_send(1, 3)
    user_chunks(1)
    to_rows(ucol, uacc)

    def spread(buf, src0, dst0, n, h, sends, recvs, k, peer):
        return remote(buf.at[pl.ds(src0, n), cols[h]], buf.at[pl.ds(dst0, n), cols[h]], sends, recvs, k, peer)

    for h in halves:
        for copy in x_in[h]:
            copy.wait_recv()
        sumz[pl.ds(base_z, 8), cols[h]] = rx[0, :, cols[h]] + rx[1, :, cols[h]] + rx[2, :, cols[h]] + rx[3, :, cols[h]]
        go([
            spread(sumz, base_z, base_z, 8, h, zsend, zrecv, 14 + 7 * h + d - 1, zpeer(d))
            for d in range(1, 8)
        ])
    mine_y = pl.multiple_of(half + base_y, 64)
    for h in halves:
        for d in range(1, 8):
            src = pl.multiple_of(lax.rem(z + 8 - d, 8) * 8, 8)
            spread(sumz, base_z, src, 8, h, zsend, zrecv, 14 + 7 * h + d - 1, zpeer(d)).wait_recv()
        total[pl.ds(mine_y, 64), cols[h]] = sumz[:, cols[h]].astype(total.dtype)
        go([
            spread(total, mine_y, mine_y, 64, h, ysend, yrecv, 6 + 3 * h + d - 1, ypeer(d))
            for d in range(1, 4)
        ])
    for h in halves:
        for d in range(1, 4):
            src = pl.multiple_of(half + lax.rem(y + 4 - d, 4) * 64, 64)
            spread(total, mine_y, src, 64, h, ysend, yrecv, 6 + 3 * h + d - 1, ypeer(d)).wait_recv()
        go([spread(total, half, half, 256, h, csend, crecv, 2 + h, sibling)])

    user_out[...] = users[...]
    uacc_out[...] = uacc[...]
    items_arrive(1)
    item_out[...] = items2[...]
    iacc_out[...] = iacc2[...]
    for h in halves:
        spread(total, half, away, 256, h, csend, crecv, 2 + h, sibling).wait_recv()
    total_out[...] = total[...]

    for turn in range(ROUNDS):
        for k in range(UH // UC):
            user_copy(turn, k, own, own).wait_send()
            grad_copy(turn, k).wait_send()
        for k in range(IH // IC):

            @pl.when(core == 0)
            def _():
                item_copy_wide(turn, k, itabs[turn]).wait_send()

            @pl.when(core == 1)
            def _():
                item_copy(turn, k).wait_send()

        accum_copy(turn, iaccs[turn]).wait_send()
    for copy in started:
        copy.wait_send()


def finish(users, uacc, items, iacc, total, racc, user_out, uacc_out, item_out, iacc_out, step_out, racc_out,
           step, accum, rcol, sems):
    copies = [
        pltpu.make_async_copy(src, dst, sems.at[k])
        for k, (src, dst) in enumerate((
            (items, item_out), (users, user_out), (uacc, uacc_out), (iacc, iacc_out),
            (step, step_out), (accum, racc_out),
        ))
    ]
    for copy in copies[:4]:
        copy.start()
    to_columns(racc, rcol)
    mean_grad = total[...].astype(F32) * (1.0 / (NB * ROUNDS))
    accum_next = rcol[:, 0:1] + jnp.mean(mean_grad * mean_grad, axis=1, keepdims=True)
    step[...] = mean_grad * lax.rsqrt(accum_next + epsilon)
    copies[4].start()
    rcol[...] = jnp.broadcast_to(accum_next, (D, 128))
    to_rows(rcol, accum)
    copies[5].start()
    for copy in copies:
        copy.wait()


def per_device(user_table, user_accum, item_table, item_accum, relation, relation_accum, targets):
    V = pltpu.VMEM
    dma = lambda *shape: pltpu.SemaphoreType.DMA(shape)
    vmem = pl.BlockSpec(memory_space=pltpu.VMEM)
    hbm = pl.BlockSpec(memory_space=pltpu.HBM)
    shapes = [((UH, D), F32), ((4, 128), F32), ((IH, D), F32), ((8, 128), F32)]
    outs = pl.pallas_call(
        kernel,
        out_shape=[jax.ShapeDtypeStruct(s, t) for s, t in shapes + [((D, D), GATHER)]],
        in_specs=[hbm] * 6,
        out_specs=[vmem] * 5,
        scratch_shapes=[
            V((UH, D), F32), V((4, 128), F32), V((IH, D), F32), V((IH, D), F32), V((IH, D), F32),
            V((8, 128), F32), V((8, 128), F32), V((8, 128), F32), V((D, D), BF),
            V((2 * UH, IH), BF), V((2 * UH, IH), BF),
            V((2 * UH, D), BF), V((2 * UH, D), BF), V((IH, D), BF), V((IH, D), BF), V((IH, D), BF),
            V((IH, D), BF), V((IH, D), BF), V((2 * UH, D), BF), V((2 * UH, IH), BF),
            V((2 * UH, D), BF), V((UH, D), F32),
            V((UH, D), BF), V((UH, D), BF), V((UH, D), BF), V((UH, D), BF),
            V((UH, 128), F32), V((IH, 128), F32), V((D, D), F32),
            V((256, D), F32), V((256, D), SCATTER), V((3, 64, D), SCATTER), V((64, D), F32), V((7, 8, D), F32),
            V((4, 8, D), F32), V((64, D), F32), V((D, D), GATHER),
            dma(7), dma(2, 4), dma(2, 4), dma(2, 4), dma(2, 4), dma(2, 4), dma(2, 4), dma(2), dma(2),
            dma(4), dma(4), dma(12), dma(12), dma(28), dma(28), dma(6), dma(6),
        ],
        compiler_params=pltpu.CompilerParams(
            collective_id=0, has_side_effects=True, vmem_limit_bytes=48 * 2**20
        ),
    )(
        *(
            pltpu.with_memory_space_constraint(v, pltpu.HBM)
            for v in (
                user_table, user_accum.reshape(4, 128), item_table, item_accum.reshape(8, 128),
                relation, targets,
            )
        )
    )
    users, uacc, items, iacc, step, racc = pl.pallas_call(
        finish,
        out_shape=[jax.ShapeDtypeStruct(s, t) for s, t in shapes + [((D, D), F32), ((4, 128), F32)]],
        in_specs=[vmem] * 6,
        out_specs=[hbm] * 6,
        scratch_shapes=[V((D, D), F32), V((4, 128), F32), V((D, 128), F32), dma(6)],
        compiler_params=pltpu.CompilerParams(vmem_limit_bytes=12 * 2**20),
    )(*outs, relation_accum.reshape(4, 128))
    return users, uacc.reshape(UH), items, iacc.reshape(IH), step, racc.reshape(D)


def solution(mesh):
    return jax.shard_map(
        per_device,
        mesh=mesh,
        in_specs=(
            P(("blk", "rel"), None),
            P(("blk", "rel")),
            P(("blk", "rel"), None),
            P(("blk", "rel")),
            P(),
            P(),
            P(None, "blk", "rel"),
        ),
        out_specs=(
            P(("blk", "rel"), None),
            P(("blk", "rel")),
            P(("blk", "rel"), None),
            P(("blk", "rel")),
            P(),
            P(),
        ),
        check_vma=False,
    )
```

```python
import jax
import jax.numpy as jnp
from jax import lax
from jax.experimental import pallas as pl
from jax.experimental.pallas import tpu as pltpu
from jax.sharding import PartitionSpec as P

learn_rate = 0.1
epsilon = 1e-06

MESH = pl.DeviceIdType.MESH
D = 512
UH = 512
IH = 1024
NB = 128
ROUNDS = 2
UC = 128
IC = 256
BF = jnp.bfloat16
F32 = jnp.float32
SCATTER = BF
GATHER = BF


def mm(a, b, ca, cb):
    return lax.dot_general(a, b, (((ca,), (cb,)), ((), ())), preferred_element_type=F32)


def to_columns(rows, cols):
    for i in range(rows.shape[0]):
        cols[i * 128 : (i + 1) * 128, :] = jnp.broadcast_to(rows[i : i + 1, :], (128, 128)).T


def to_rows(cols, rows):
    for i in range(rows.shape[0]):
        rows[i : i + 1, :] = cols[i * 128 : (i + 1) * 128, :].T[0:1, :]


def adagrad(table, accum, grads):
    accum_next = accum + jnp.mean(grads * grads, axis=1, keepdims=True)
    return table - learn_rate * grads * lax.rsqrt(accum_next + epsilon), accum_next


def kernel(
    user_in, uacc_in, item_in, iacc_in, rel_in, tgt_in,
    user_out, uacc_out, item_out, iacc_out, total_out,
    users, uacc, items0, items1, items2, iacc0, iacc1, iacc2, rel, tgt0, tgt1,
    ub0, ub1, vb0, vb1, vb2, vtx0, vtx1, anchor, errors, wsum, ugown,
    gtx0, gtx1, grx0, grx1, ucol, icol, term, rcore, mine, ry, sumy, rz, rx, sumz, total,
    load, usend, urecv, gsend, grecv, isend, irecv, asend, arecv,
    csend, crecv, ysend, yrecv, zsend, zrecv, xsend, xrecv,
):
    b = lax.axis_index("blk")
    r = lax.axis_index("rel")
    core = lax.rem(b, 2)
    xlo = lax.rem(b // 2, 2)
    z = lax.rem(b // 4, 8)
    y = b // 32
    x = 2 * r + xlo
    partner = (b, 1 - r)
    sibling = (b + 1 - 2 * core, r)
    other = (lax.rem(b + 2 * core + (NB - 1), NB), r)
    nxt = (lax.rem(b + 1, NB), r)

    def xpeer(d):
        xp = lax.rem(x + d, 4)
        return (b - 2 * xlo + 2 * lax.rem(xp, 2), xp // 2)

    def ypeer(d):
        return (b - 32 * y + 32 * lax.rem(y + d, 4), r)

    def zpeer(d):
        return (b - 4 * z + 4 * lax.rem(z + d, 8), r)

    barrier = pltpu.get_barrier_semaphore()
    greet = [xpeer(d) for d in range(1, 4)] + [ypeer(d) for d in range(1, 4)]
    greet += [zpeer(d) for d in range(1, 8)] + [sibling, other]
    for peer in greet:
        pl.semaphore_signal(barrier, inc=1, device_id=peer, device_id_type=MESH)

    loads = []
    for src, dst in (
        (user_in, users), (rel_in, rel), (item_in, items0), (tgt_in.at[0], tgt0),
        (uacc_in, uacc), (iacc_in, iacc0), (tgt_in.at[1], tgt1),
    ):
        copy = pltpu.make_async_copy(src, dst, load.at[len(loads)])
        copy.start()
        loads.append(copy)

    own = pl.multiple_of(r * UH, UH)
    far = pl.multiple_of((1 - r) * UH, UH)

    ubs, vbs, vtxs = (ub0, ub1), (vb0, vb1), (vtx0, vtx1)
    tgts, gtxs, grxs = (tgt0, tgt1), (gtx0, gtx1), (grx0, grx1)
    itabs, iaccs, vins = (items0, items1, items2), (iacc0, iacc1, iacc2), (vb0, vb1, vb2)

    def user_copy(turn, k, src0, dst0):
        return pltpu.make_async_remote_copy(
            ubs[turn].at[pl.ds(src0 + k * UC, UC)], ubs[turn].at[pl.ds(dst0 + k * UC, UC)],
            usend.at[turn, k], urecv.at[turn, k], device_id=partner, device_id_type=MESH,
        )

    def grad_copy(turn, k):
        rows = pl.ds(k * UC, UC)
        return pltpu.make_async_remote_copy(
            gtxs[turn].at[rows], grxs[turn].at[rows],
            gsend.at[turn, k], grecv.at[turn, k], device_id=partner, device_id_type=MESH,
        )

    def item_copy_wide(turn, k, src):
        rows = pl.ds(k * IC, IC)
        return pltpu.make_async_remote_copy(
            src.at[rows], itabs[turn + 1].at[rows],
            isend.at[turn, k], irecv.at[turn, k], device_id=nxt, device_id_type=MESH,
        )

    def item_copy(turn, k):
        rows = pl.ds(k * IC, IC)
        return pltpu.make_async_remote_copy(
            vtxs[turn].at[rows], vins[turn + 1].at[rows],
            isend.at[turn, k], irecv.at[turn, k], device_id=nxt, device_id_type=MESH,
        )

    def accum_copy(turn, src):
        return pltpu.make_async_remote_copy(
            src, iaccs[turn + 1], asend.at[turn], arecv.at[turn],
            device_id=nxt, device_id_type=MESH,
        )

    def score_rows(turn, row0, n):
        rows = pl.ds(row0, n)
        anc = mm(ubs[turn][rows, :], rel[...], 1, 0).astype(BF)
        anchor[rows, :] = anc
        scores = mm(anc, vbs[turn][...], 1, 1)
        err = (0.5 * jnp.tanh(0.5 * scores) + 0.5 - tgts[turn][rows, :].astype(F32)).astype(BF)
        errors[rows, :] = err
        w = mm(err, vbs[turn][...], 1, 0).astype(BF)
        wsum[rows, :] = w
        return mm(w, rel[...], 1, 1)

    def own_rows(turn):
        def step(k, carry):
            row0 = pl.multiple_of(k * 256, 256)
            ugown[pl.ds(row0, 256), :] = score_rows(turn, pl.multiple_of(own + row0, 256), 256)
            return carry

        lax.fori_loop(0, UH // 256, step, 0)

    def far_rows(turn):
        def step(k, carry):
            user_copy(turn, k, own, far).wait_recv()
            row0 = pl.multiple_of(k * UC, UC)
            grad = score_rows(turn, pl.multiple_of(far + row0, UC), UC)
            gtxs[turn][pl.ds(row0, UC), :] = grad.astype(BF)
            grad_copy(turn, k).start()
            return carry

        lax.fori_loop(0, UH // UC, step, 0)

    def add_term(turn, row0, first):
        rows = pl.ds(row0, UH)
        part = mm(ubs[turn][rows, :], wsum[rows, :], 0, 0)
        term[...] = part if first else term[...] + part

    def item_update(turn, k):
        rows = pl.ds(k * IC, IC)
        grad = mm(errors[:, k * IC : (k + 1) * IC], anchor[...], 0, 0)
        new, acc = adagrad(itabs[turn][rows, :], icol[rows, 0:1], grad)
        icol[rows, :] = jnp.broadcast_to(acc, (IC, 128))
        itabs[turn][rows, :] = new
        vtxs[turn][rows, :] = new.astype(BF)

    def item_send(turn, k):
        @pl.when(core == 0)
        def _():
            item_copy_wide(turn, k, itabs[turn]).start()

        @pl.when(core == 1)
        def _():
            item_copy(turn, k).start()

    def user_chunks(turn):
        def step(k, carry):
            grad_copy(turn, k).wait_recv()
            row0 = pl.multiple_of(k * UC, UC)
            rows = pl.ds(row0, UC)
            grad = ugown[rows, :] + grxs[turn][rows, :].astype(F32)
            new, acc = adagrad(users[rows, :], ucol[rows, 0:1], grad)
            ucol[rows, :] = jnp.broadcast_to(acc, (UC, 128))
            users[rows, :] = new
            if turn + 1 < ROUNDS:
                ubs[turn + 1][pl.ds(pl.multiple_of(own + row0, UC), UC), :] = new.astype(BF)
                user_copy(turn + 1, k, own, own).start()
            return carry

        lax.fori_loop(0, UH // UC, step, 0)

    def items_arrive(turn):
        def step(k, carry):
            row0 = pl.multiple_of(k * IC, IC)
            rows = pl.ds(row0, IC)

            @pl.when(core == 0)
            def _():
                item_copy(turn, k).wait_recv()
                itabs[turn + 1][rows, :] = vins[turn + 1][rows, :].astype(F32)

            @pl.when(core == 1)
            def _():
                item_copy_wide(turn, k, itabs[turn]).wait_recv()
                if turn + 1 < ROUNDS:
                    vins[turn + 1][rows, :] = itabs[turn + 1][rows, :].astype(BF)

            return carry

        lax.fori_loop(0, IH // IC, step, 0)
        accum_copy(turn, iaccs[turn]).wait_recv()

    loads[0].wait()
    ub0[pl.ds(own, UH), :] = users[...].astype(BF)
    pl.semaphore_wait(barrier, len(greet))
    for k in range(UH // UC):
        user_copy(0, k, own, own).start()
    for copy in loads[1:6]:
        copy.wait()
    vb0[...] = items0[...].astype(BF)
    to_columns(uacc, ucol)
    to_columns(iacc0, icol)
    own_rows(0)
    add_term(0, own, True)
    far_rows(0)
    for k in range(IH // IC):
        item_update(0, k)
        item_send(0, k)
    to_rows(icol, iacc0)
    accum_copy(0, iacc0).start()
    user_chunks(0)
    add_term(0, far, False)
    loads[6].wait()

    items_arrive(0)
    to_columns(iacc1, icol)
    own_rows(1)
    add_term(1, own, False)
    far_rows(1)
    add_term(1, far, False)

    half = pl.multiple_of(core * 256, 256)
    away = pl.multiple_of(256 - core * 256, 256)
    base_y = pl.multiple_of(y * 64, 64)
    base_z = pl.multiple_of(z * 8, 8)
    started = []

    def remote(src, dst, sends, recvs, k, peer):
        return pltpu.make_async_remote_copy(
            src, dst, sends.at[k], recvs.at[k], device_id=peer, device_id_type=MESH
        )

    def go(copies):
        for copy in copies:
            copy.start()
        started.extend(copies)
        return copies

    halves = range(2)
    cols = [pl.ds(h * 256, 256) for h in halves]
    core_in = go([
        remote(term.at[pl.ds(away, 256), cols[h]], rcore.at[:, cols[h]], csend, crecv, h, sibling)
        for h in halves
    ])
    item_update(1, 0)
    item_send(1, 0)
    y_in = []
    for h in halves:
        core_in[h].wait_recv()
        both = term[pl.ds(half, 256), cols[h]] + rcore[:, cols[h]]
        mine[:, cols[h]] = both.astype(mine.dtype)
        y_in.append(go([
            remote(
                mine.at[pl.ds(pl.multiple_of(lax.rem(y + d, 4) * 64, 64), 64), cols[h]],
                ry.at[d - 1, :, cols[h]], ysend, yrecv, 3 * h + d - 1, ypeer(d),
            )
            for d in range(1, 4)
        ]))
    item_update(1, 1)
    item_send(1, 1)
    item_update(1, 2)
    item_update(1, 3)
    to_rows(icol, iacc1)
    accum_copy(1, iacc1).start()
    z_in = []
    for h in halves:
        for copy in y_in[h]:
            copy.wait_recv()
        part = mine[pl.ds(base_y, 64), cols[h]].astype(F32)
        for d in range(3):
            part = part + ry[d, :, cols[h]].astype(F32)
        sumy[:, cols[h]] = part
        z_in.append(go([
            remote(
                sumy.at[pl.ds(pl.multiple_of(lax.rem(z + d, 8) * 8, 8), 8), cols[h]],
                rz.at[d - 1, :, cols[h]], zsend, zrecv, 7 * h + d - 1, zpeer(d),
            )
            for d in range(1, 8)
        ]))
    x_in = []
    for h in halves:
        for copy in z_in[h]:
            copy.wait_recv()
        part = sumy[pl.ds(base_z, 8), cols[h]]
        for d in range(7):
            part = part + rz[d, :, cols[h]]
        rx[pl.ds(x, 1), :, cols[h]] = part[None]
        go([
            remote(rx.at[x, :, cols[h]], rx.at[x, :, cols[h]], xsend, xrecv, 3 * h + d - 1, xpeer(d))
            for d in range(1, 4)
        ])
        x_in.append([
            remote(
                rx.at[x, :, cols[h]], rx.at[lax.rem(x + 4 - d, 4), :, cols[h]],
                xsend, xrecv, 3 * h + d - 1, xpeer(d),
            )
            for d in range(1, 4)
        ])
    item_send(1, 2)

    def spread(buf, src0, dst0, n, h, sends, recvs, k, peer):
        return remote(buf.at[pl.ds(src0, n), cols[h]], buf.at[pl.ds(dst0, n), cols[h]], sends, recvs, k, peer)

    for h in halves:
        for copy in x_in[h]:
            copy.wait_recv()
        sumz[pl.ds(base_z, 8), cols[h]] = rx[0, :, cols[h]] + rx[1, :, cols[h]] + rx[2, :, cols[h]] + rx[3, :, cols[h]]
        go([
            spread(sumz, base_z, base_z, 8, h, zsend, zrecv, 14 + 7 * h + d - 1, zpeer(d))
            for d in range(1, 8)
        ])
    item_send(1, 3)
    mine_y = pl.multiple_of(half + base_y, 64)
    for h in halves:
        for d in range(1, 8):
            src = pl.multiple_of(lax.rem(z + 8 - d, 8) * 8, 8)
            spread(sumz, base_z, src, 8, h, zsend, zrecv, 14 + 7 * h + d - 1, zpeer(d)).wait_recv()
        total[pl.ds(mine_y, 64), cols[h]] = sumz[:, cols[h]].astype(total.dtype)
        go([
            spread(total, mine_y, mine_y, 64, h, ysend, yrecv, 6 + 3 * h + d - 1, ypeer(d))
            for d in range(1, 4)
        ])
    user_chunks(1)
    to_rows(ucol, uacc)
    user_out[...] = users[...]
    uacc_out[...] = uacc[...]
    for h in halves:
        for d in range(1, 4):
            src = pl.multiple_of(half + lax.rem(y + 4 - d, 4) * 64, 64)
            spread(total, mine_y, src, 64, h, ysend, yrecv, 6 + 3 * h + d - 1, ypeer(d)).wait_recv()
        go([spread(total, half, half, 256, h, csend, crecv, 2 + h, sibling)])

    items_arrive(1)
    item_out[...] = items2[...]
    iacc_out[...] = iacc2[...]
    for h in halves:
        spread(total, half, away, 256, h, csend, crecv, 2 + h, sibling).wait_recv()
    total_out[...] = total[...]

    for turn in range(ROUNDS):
        for k in range(UH // UC):
            user_copy(turn, k, own, own).wait_send()
            grad_copy(turn, k).wait_send()
        for k in range(IH // IC):

            @pl.when(core == 0)
            def _():
                item_copy_wide(turn, k, itabs[turn]).wait_send()

            @pl.when(core == 1)
            def _():
                item_copy(turn, k).wait_send()

        accum_copy(turn, iaccs[turn]).wait_send()
    for copy in started:
        copy.wait_send()


def finish(users, uacc, items, iacc, total, racc, user_out, uacc_out, item_out, iacc_out, step_out, racc_out,
           step, accum, rcol, sems):
    copies = [
        pltpu.make_async_copy(src, dst, sems.at[k])
        for k, (src, dst) in enumerate((
            (items, item_out), (users, user_out), (uacc, uacc_out), (iacc, iacc_out),
            (step, step_out), (accum, racc_out),
        ))
    ]
    for copy in copies[:4]:
        copy.start()
    to_columns(racc, rcol)
    mean_grad = total[...].astype(F32) * (1.0 / (NB * ROUNDS))
    accum_next = rcol[:, 0:1] + jnp.mean(mean_grad * mean_grad, axis=1, keepdims=True)
    step[...] = mean_grad * lax.rsqrt(accum_next + epsilon)
    copies[4].start()
    rcol[...] = jnp.broadcast_to(accum_next, (D, 128))
    to_rows(rcol, accum)
    copies[5].start()
    for copy in copies:
        copy.wait()


def per_device(user_table, user_accum, item_table, item_accum, relation, relation_accum, targets):
    V = pltpu.VMEM
    dma = lambda *shape: pltpu.SemaphoreType.DMA(shape)
    vmem = pl.BlockSpec(memory_space=pltpu.VMEM)
    hbm = pl.BlockSpec(memory_space=pltpu.HBM)
    shapes = [((UH, D), F32), ((4, 128), F32), ((IH, D), F32), ((8, 128), F32)]
    outs = pl.pallas_call(
        kernel,
        out_shape=[jax.ShapeDtypeStruct(s, t) for s, t in shapes + [((D, D), GATHER)]],
        in_specs=[hbm] * 6,
        out_specs=[vmem] * 5,
        scratch_shapes=[
            V((UH, D), F32), V((4, 128), F32), V((IH, D), F32), V((IH, D), F32), V((IH, D), F32),
            V((8, 128), F32), V((8, 128), F32), V((8, 128), F32), V((D, D), BF),
            V((2 * UH, IH), BF), V((2 * UH, IH), BF),
            V((2 * UH, D), BF), V((2 * UH, D), BF), V((IH, D), BF), V((IH, D), BF), V((IH, D), BF),
            V((IH, D), BF), V((IH, D), BF), V((2 * UH, D), BF), V((2 * UH, IH), BF),
            V((2 * UH, D), BF), V((UH, D), F32),
            V((UH, D), BF), V((UH, D), BF), V((UH, D), BF), V((UH, D), BF),
            V((UH, 128), F32), V((IH, 128), F32), V((D, D), F32),
            V((256, D), F32), V((256, D), SCATTER), V((3, 64, D), SCATTER), V((64, D), F32), V((7, 8, D), F32),
            V((4, 8, D), F32), V((64, D), F32), V((D, D), GATHER),
            dma(7), dma(2, 4), dma(2, 4), dma(2, 4), dma(2, 4), dma(2, 4), dma(2, 4), dma(2), dma(2),
            dma(4), dma(4), dma(12), dma(12), dma(28), dma(28), dma(6), dma(6),
        ],
        compiler_params=pltpu.CompilerParams(
            collective_id=0, has_side_effects=True, vmem_limit_bytes=48 * 2**20
        ),
    )(
        *(
            pltpu.with_memory_space_constraint(v, pltpu.HBM)
            for v in (
                user_table, user_accum.reshape(4, 128), item_table, item_accum.reshape(8, 128),
                relation, targets,
            )
        )
    )
    users, uacc, items, iacc, step, racc = pl.pallas_call(
        finish,
        out_shape=[jax.ShapeDtypeStruct(s, t) for s, t in shapes + [((D, D), F32), ((4, 128), F32)]],
        in_specs=[vmem] * 6,
        out_specs=[hbm] * 6,
        scratch_shapes=[V((D, D), F32), V((4, 128), F32), V((D, 128), F32), dma(6)],
        compiler_params=pltpu.CompilerParams(vmem_limit_bytes=12 * 2**20),
    )(*outs, relation_accum.reshape(4, 128))
    return users, uacc.reshape(UH), items, iacc.reshape(IH), step, racc.reshape(D)


def solution(mesh):
    return jax.shard_map(
        per_device,
        mesh=mesh,
        in_specs=(
            P(("blk", "rel"), None),
            P(("blk", "rel")),
            P(("blk", "rel"), None),
            P(("blk", "rel")),
            P(),
            P(),
            P(None, "blk", "rel"),
        ),
        out_specs=(
            P(("blk", "rel"), None),
            P(("blk", "rel")),
            P(("blk", "rel"), None),
            P(("blk", "rel")),
            P(),
            P(),
        ),
        check_vma=False,
    )
```
